8 devices in a mesh: dp: 1 (over z), sp: 8 (over y, x, core).
Axes of the slice: x: 2, y: 2, z: 1, core: 2. Of those that a mesh axis runs over, the one named last changes fastest.
Arguments:
- hidden: bfloat16 [512, 2048], P('dp')
- w_norm: bfloat16 [2048], replicated
- w_q: bfloat16 [2048, 2048], replicated
- w_k: bfloat16 [2048, 256], replicated
- w_v: bfloat16 [2048, 256], replicated
- w_o: bfloat16 [2048, 2048], replicated
- k_cache: bfloat16 [512, 1024, 256], P('dp', 'sp')
- v_cache: bfloat16 [512, 1024, 256], P('dp', 'sp')
- cache_len: int32 [512], P('dp')
Outputs:
- output 1: bfloat16 [512, 2048], P('dp')
- output 2: bfloat16 [512, 1024, 256], P('dp', 'sp')
- output 3: bfloat16 [512, 1024, 256], P('dp', 'sp')
All inputs are finite; a program needn't handle non-finite values.
Results may differ from the reference program's by a relative error of at most 0.0133847.
Values sent between devices are 32-bit elements.
A program may use at most 1 GiB of HBM per device.

```python
import math
import jax
import jax.numpy as jnp
from jax import lax

D = 2048
HEADS = 8
HEAD = 256
ROWS = 512
SEQ = 1024

ROPE_BASE = 10000.0
EPSILON = 1e-6


def rotate_half(vectors, cos_t, sin_t):
    half_dim = vectors.shape[-1] // 2
    lower_half = vectors[..., :half_dim]
    upper_half = vectors[..., half_dim:]
    return jnp.concatenate([lower_half * cos_t - upper_half * sin_t, upper_half * cos_t + lower_half * sin_t], axis=-1)


def setup_inputs(seed: int = 0, part: int = 0) -> dict:
    base_key = jax.random.key(seed)
    shared_keys = jax.random.split(base_key, 5)
    part_keys = jax.random.split(jax.random.fold_in(base_key, part), 5)
    width = HEADS * HEAD
    score_spread = math.sqrt(max(math.log(SEQ / 16.0), 1.0))
    align = (1.5 * math.log(SEQ) - 3.5) * HEADS / math.sqrt(HEAD)
    hidden = jax.random.normal(part_keys[0], (ROWS, D), jnp.float32)
    w_norm = 0.5 * jax.random.normal(shared_keys[0], (D,), jnp.float32)
    w_q = jax.random.normal(shared_keys[1], (D, width), jnp.float32) * D ** -0.5
    q_mean = w_q.reshape(D, HEADS, HEAD).mean(axis=1)
    w_k = align * q_mean + jax.random.normal(shared_keys[2], (D, HEAD), jnp.float32) * D ** -0.5
    w_v = jax.random.normal(shared_keys[3], (D, HEAD), jnp.float32) * D ** -0.5
    w_o = jax.random.normal(shared_keys[4], (width, D), jnp.float32) * (3.0 * width ** -0.5)
    key_scale = score_spread * jax.random.uniform(part_keys[1], (ROWS, SEQ, 1), jnp.float32, minval=0.5, maxval=1.5)
    k_cache = jax.random.normal(part_keys[2], (ROWS, SEQ, HEAD), jnp.float32) * key_scale
    v_cache = jax.random.normal(part_keys[3], (ROWS, SEQ, HEAD), jnp.float32)
    row_ids = jnp.arange(ROWS)
    lengths = jax.random.randint(part_keys[4], (ROWS,), SEQ // 8, SEQ)
    lengths = jnp.where(row_ids == 0, SEQ - 1, jnp.where(row_ids == ROWS - 1, SEQ // 8, lengths))
    return {'hidden': hidden.astype(jnp.bfloat16), 'w_norm': w_norm.astype(jnp.bfloat16), 'w_q': w_q.astype(jnp.bfloat16), 'w_k': w_k.astype(jnp.bfloat16), 'w_v': w_v.astype(jnp.bfloat16), 'w_o': w_o.astype(jnp.bfloat16), 'k_cache': k_cache.astype(jnp.bfloat16), 'v_cache': v_cache.astype(jnp.bfloat16), 'cache_len': lengths.astype(jnp.int32)}


def reference(hidden, w_norm, w_q, w_k, w_v, w_o, k_cache, v_cache, cache_len):
    x_f32 = hidden.astype(jnp.float32)
    inv_rms = lax.rsqrt(jnp.mean(x_f32 * x_f32, axis=-1, keepdims=True) + EPSILON)
    x_norm = (x_f32 * inv_rms * (1.0 + w_norm.astype(jnp.float32))).astype(jnp.bfloat16)
    q_proj = jnp.dot(x_norm, w_q, preferred_element_type=jnp.float32).astype(jnp.bfloat16)
    k_proj = jnp.dot(x_norm, w_k, preferred_element_type=jnp.float32).astype(jnp.bfloat16)
    v_proj = jnp.dot(x_norm, w_v, preferred_element_type=jnp.float32).astype(jnp.bfloat16)
    inv_freq = ROPE_BASE ** (-jnp.arange(HEAD // 2, dtype=jnp.float32) * 2.0 / HEAD)
    angles = cache_len.astype(jnp.float32)[:, None] * inv_freq[None, :]
    cos_t = jnp.cos(angles)
    sin_t = jnp.sin(angles)
    q_heads = q_proj.astype(jnp.float32).reshape(ROWS, HEADS, HEAD)
    q_rot = (rotate_half(q_heads, cos_t[:, None, :], sin_t[:, None, :]) * HEAD ** -0.5).astype(jnp.bfloat16)
    k_rot = rotate_half(k_proj.astype(jnp.float32), cos_t, sin_t).astype(jnp.bfloat16)
    positions = jnp.arange(SEQ)
    at_slot = (positions[None, :] == cache_len[:, None])[:, :, None]
    new_k_cache = jnp.where(at_slot, k_rot[:, None, :], k_cache)
    new_v_cache = jnp.where(at_slot, v_proj[:, None, :], v_cache)

    def one_row(row_args):
        q_row, k_row, v_row, length = row_args
        scores = jnp.einsum('hd,td->ht', q_row.astype(jnp.float32), k_row.astype(jnp.float32))
        scores = jnp.where(positions[None, :] <= length, scores, -jnp.inf)
        weights = jax.nn.softmax(scores, axis=-1)
        return jnp.einsum('ht,td->hd', weights, v_row.astype(jnp.float32))

    attended = lax.map(one_row, (q_rot, new_k_cache, new_v_cache, cache_len))
    attended = attended.reshape(ROWS, HEADS * HEAD).astype(jnp.bfloat16)
    out_hidden = x_f32 + jnp.dot(attended, w_o, preferred_element_type=jnp.float32)
    return out_hidden.astype(jnp.bfloat16), new_k_cache, new_v_cache
```

```python
import functools
import jax
import jax.numpy as jnp
from jax import lax
from jax.experimental import pallas as pl
from jax.experimental.pallas import tpu as pltpu
from jax.sharding import PartitionSpec as P

ROPE_BASE = 10000.0
EPSILON = 1e-6
F32 = jnp.float32
BF16 = jnp.bfloat16
LOWEST = -3.0e38
MESH_ID = pl.DeviceIdType.MESH

ROWS, D, HEADS, HEAD, SLOTS = 512, 2048, 8, 256, 128
CHUNK = 128
N_CHUNKS = ROWS // CHUNK
GROUP = 16
N_GROUPS = ROWS // GROUP
G_PER_CHUNK = CHUNK // GROUP
RING = 8
EIGHTH = CHUNK // 8


def place(me):
    core = me % 2
    x = (me // 2) % 2
    y = me // 4
    partner = me + 1 - 2 * core
    x_peer = me + 2 * (1 - 2 * x)
    y_peer = me + 4 * (1 - 2 * y)
    first_bit = x + core * (y - x)
    second_bit = y + core * (x - y)
    first_peer = x_peer + core * (y_peer - x_peer)
    second_peer = y_peer + core * (x_peer - y_peer)
    return core, first_bit, second_bit, partner, first_peer, second_peer


def eighth_of(me):
    core, first_bit, second_bit, _, _, _ = place(me)
    return core * 4 + first_bit * 2 + second_bit


def dot(a, b):
    return jnp.dot(a, b, preferred_element_type=F32)


def attend_kernel(x_ref, wn_ref, cos_ref, sin_ref, len_ref, wq_hbm, wk_hbm, wv_hbm, wo_hbm, k_hbm, v_hbm,
                  out_ref, knew_ref, vnew_ref,
                  w_buf, wkv_buf, xn_buf, q_buf, k_buf, v_buf, num_buf, stat_buf, d_recv, f_recv, s_recv,
                  d_stat, f_stat, s_stat, att_buf, w_sem, wkv_sem, k_sem, v_sem, send_sem, recv_sem, ssend_sem, srecv_sem):
    me = lax.axis_index('sp')
    core, first_bit, second_bit, partner, first_peer, second_peer = place(me)
    base = me * SLOTS

    def wq_copy(h):
        cols = pl.ds(pl.multiple_of(h * HEAD, HEAD), HEAD)
        return pltpu.make_async_copy(wq_hbm.at[:, cols], w_buf.at[:, cols], w_sem.at[h])

    def wo_copy(h):
        rows = pl.ds(pl.multiple_of(h * HEAD, HEAD), HEAD)
        return pltpu.make_async_copy(wo_hbm.at[rows, :], w_buf.at[rows, :], w_sem.at[h])

    def cache_copies(g):
        slot = g % RING
        rows = pl.ds(g * GROUP, GROUP)
        return (pltpu.make_async_copy(k_hbm.at[rows], k_buf.at[slot], k_sem.at[slot]),
                pltpu.make_async_copy(v_hbm.at[rows], v_buf.at[slot], v_sem.at[slot]))

    wk_copy = pltpu.make_async_copy(wk_hbm, wkv_buf.at[0], wkv_sem.at[0])
    wv_copy = pltpu.make_async_copy(wv_hbm, wkv_buf.at[1], wkv_sem.at[1])
    for h in range(2):
        wq_copy(h).start()
    wk_copy.start()
    wv_copy.start()
    for h in range(2, HEADS):
        wq_copy(h).start()
    for g in range(RING):
        for copy in cache_copies(g):
            copy.start()

    barrier = pltpu.get_barrier_semaphore()
    for peer in (partner, first_peer, second_peer):
        pl.semaphore_signal(barrier, inc=1, device_id={'sp': peer}, device_id_type=MESH_ID)
    pl.semaphore_wait(barrier, 3)

    gain = 1.0 + wn_ref[...].astype(F32)

    @pl.loop(0, ROWS // 16)
    def _(i):
        rows = pl.ds(pl.multiple_of(i * 16, 16), 16)
        x = x_ref[rows, :].astype(F32)
        inv = lax.rsqrt(jnp.mean(x * x, axis=-1, keepdims=True) + EPSILON)
        xn_buf[rows, :] = (x * inv * gain).astype(BF16)

    def rotate(u, rows):
        u = u.astype(BF16).astype(F32)
        c, s = cos_ref[rows, :], sin_ref[rows, :]
        lo, hi = u[:, :HEAD // 2], u[:, HEAD // 2:]
        return lo * c - hi * s, hi * c + lo * s

    half = HEAD // 2
    row_tiles = [pl.ds(t * 256, 256) for t in range(ROWS // 256)]

    @pl.loop(0, HEADS)
    def _(h):
        wq_copy(h).wait()
        cols = pl.ds(pl.multiple_of(h * HEAD, HEAD), HEAD)
        for t, rows in enumerate(row_tiles):
            lo, hi = rotate(dot(xn_buf[rows, :], w_buf[:, cols]), rows)
            dst = pl.ds(t * 256 * HEADS + h, 256, stride=HEADS)
            q_buf[0, dst, :] = lo * HEAD ** -0.5
            q_buf[1, dst, :] = hi * HEAD ** -0.5

    wk_copy.wait()
    for rows in row_tiles:
        lo, hi = rotate(dot(xn_buf[rows, :], wkv_buf[0]), rows)
        knew_ref[rows, :half] = lo.astype(BF16).astype(F32)
        knew_ref[rows, half:] = hi.astype(BF16).astype(F32)
    wv_copy.wait()
    for rows in row_tiles:
        vnew_ref[rows, :] = dot(xn_buf[rows, :], wkv_buf[1]).astype(BF16).astype(F32)

    for h in range(HEADS):
        wo_copy(h).start()

    lane = lax.broadcasted_iota(jnp.int32, (HEADS, SLOTS), 1)
    sub16 = lax.broadcasted_iota(jnp.int32, (16, HEAD), 0).astype(F32).astype(BF16)

    def patched(ref, slot, j, new_row, lim):
        new = jnp.broadcast_to(new_row, (16, HEAD)).astype(BF16)
        tiles = []
        for t in range(SLOTS // 16):
            at = jnp.full((16, HEAD), (lim - t * 16).astype(F32), F32).astype(BF16)
            tiles.append(jnp.where(sub16 == at, new, ref[slot, j, t * 16:(t + 1) * 16, :]))
        return jnp.concatenate(tiles, axis=0)

    def attend_group(g):
        slot = g % RING
        for copy in cache_copies(g):
            copy.wait()
        chunk = g // G_PER_CHUNK
        m_tile = stat_buf[chunk, 0]
        d_tile = stat_buf[chunk, 1]
        for pair in range(GROUP // 2):
            r0 = g * GROUP + 2 * pair
            lims = [len_ref[r0 + a] - base for a in range(2)]
            keys = jnp.concatenate([patched(k_buf, slot, 2 * pair + a, knew_ref[pl.ds(r0 + a, 1), :], lims[a]) for a in range(2)], axis=0)
            q_rows = pl.ds(pl.multiple_of(r0 * HEADS, 16), 16)
            q2 = jnp.concatenate([q_buf[0, q_rows, :], q_buf[1, q_rows, :]], axis=1).astype(BF16)
            s2 = lax.dot_general(q2, keys, (((1,), (1,)), ((), ())), preferred_element_type=F32)
            probs = []
            for a in range(2):
                s = s2[a * HEADS:(a + 1) * HEADS, a * SLOTS:(a + 1) * SLOTS]
                valid = lane <= lims[a]
                m = jnp.max(jnp.where(valid, s, LOWEST), axis=-1, keepdims=True)
                p = jnp.where(valid, jnp.exp(s - m), 0.0)
                den = jnp.sum(p, axis=-1, keepdims=True)
                here = lane == (g % G_PER_CHUNK) * GROUP + 2 * pair + a
                m_tile = jnp.where(here, m, m_tile)
                d_tile = jnp.where(here, den, d_tile)
                probs.append(p)
            zero = jnp.zeros((HEADS, SLOTS), F32)
            p2 = jnp.concatenate([jnp.concatenate([probs[0], zero], axis=1), jnp.concatenate([zero, probs[1]], axis=1)], axis=0).astype(BF16)
            values = jnp.concatenate([patched(v_buf, slot, 2 * pair + a, vnew_ref[pl.ds(r0 + a, 1), :], lims[a]) for a in range(2)], axis=0)
            num_buf[pl.ds(pl.multiple_of(r0 * HEADS, 16), 16), :] = dot(p2, values)
        stat_buf[chunk, 0] = m_tile
        stat_buf[chunk, 1] = d_tile

        @pl.when(g + RING < N_GROUPS)
        def _():
            for copy in cache_copies(g + RING):
                copy.start()

    def num_rows(k, offset, count):
        return pl.ds(pl.multiple_of((k * CHUNK + offset) * HEADS, 128), count * HEADS)

    half_rows, quarter_rows = CHUNK // 2, CHUNK // 4
    my_half = core * half_rows
    my_quarter = my_half + first_bit * quarter_rows
    my_eighth = my_quarter + second_bit * EIGHTH

    def exchange(stage, k):
        recv, stat, peer, offset, count = (
            (d_recv, d_stat, partner, (1 - core) * half_rows, half_rows),
            (f_recv, f_stat, first_peer, my_half + (1 - first_bit) * quarter_rows, quarter_rows),
            (s_recv, s_stat, second_peer, my_quarter + (1 - second_bit) * EIGHTH, EIGHTH))[stage]
        return (pltpu.make_async_remote_copy(
                    src_ref=num_buf.at[num_rows(k, offset, count), :], dst_ref=recv.at[k],
                    send_sem=send_sem.at[stage, k], recv_sem=recv_sem.at[stage, k],
                    device_id={'sp': peer}, device_id_type=MESH_ID),
                pltpu.make_async_remote_copy(
                    src_ref=stat_buf.at[stage * N_CHUNKS + k], dst_ref=stat.at[k],
                    send_sem=ssend_sem.at[stage, k], recv_sem=srecv_sem.at[stage, k],
                    device_id={'sp': peer}, device_id_type=MESH_ID))

    def merge(stage, k):
        recv, stat, offset, count = (
            (d_recv, d_stat, my_half, half_rows),
            (f_recv, f_stat, my_quarter, quarter_rows),
            (s_recv, s_stat, my_eighth, EIGHTH))[stage]
        for copy in exchange(stage, k):
            copy.wait_recv()
        m_a, d_a = stat_buf[stage * N_CHUNKS + k, 0], stat_buf[stage * N_CHUNKS + k, 1]
        m_b, d_b = stat[k, 0], stat[k, 1]
        m = jnp.maximum(m_a, m_b)
        f_a, f_b = jnp.exp(m_a - m), jnp.exp(m_b - m)
        den = d_a * f_a + d_b * f_b
        last = stage == 2
        if last:
            f_a, f_b = f_a / den, f_b / den
        else:
            stat_buf[(stage + 1) * N_CHUNKS + k, 0] = m
            stat_buf[(stage + 1) * N_CHUNKS + k, 1] = den
        shift = (CHUNK - offset) % CHUNK
        f_a = pltpu.roll(f_a, shift, 1)
        f_b = pltpu.roll(f_b, shift, 1)
        start = (k * CHUNK + offset) * HEADS
        for r in range(count):
            dst = pl.ds(pl.multiple_of(start + r * HEADS, HEADS), HEADS)
            total = num_buf[dst, :] * f_a[:, r:r + 1] + recv[k, r * HEADS:(r + 1) * HEADS, :] * f_b[:, r:r + 1]
            if last:
                att_buf[0, r * HEADS:(r + 1) * HEADS, :] = total[:, :half]
                att_buf[1, r * HEADS:(r + 1) * HEADS, :] = total[:, half:]
            else:
                num_buf[dst, :] = total

    def send(stage, k):
        for copy in exchange(stage, k):
            copy.start()

    def project_out(k):
        atts = []
        for h in range(HEADS):
            heads = pl.ds(h, EIGHTH, stride=HEADS)
            atts.append(jnp.concatenate([att_buf[0, heads, :], att_buf[1, heads, :]], axis=1).astype(BF16))
        x_rows = pl.ds(pl.multiple_of(k * CHUNK + my_eighth, EIGHTH), EIGHTH)
        o_rows = pl.ds(pl.multiple_of(k * EIGHTH, EIGHTH), EIGHTH)
        for n in range(D // 512):
            cols = slice(n * 512, (n + 1) * 512)
            acc = dot(atts[0], w_buf[0:HEAD, cols])
            for h in range(1, HEADS):
                acc += dot(atts[h], w_buf[h * HEAD:(h + 1) * HEAD, cols])
            out_ref[o_rows, cols] = (x_ref[x_rows, cols].astype(F32) + acc).astype(BF16).astype(F32)

    @pl.loop(0, N_CHUNKS + 3)
    def _(t):
        @pl.when(t < N_CHUNKS)
        def _():
            @pl.loop(0, G_PER_CHUNK // 2)
            def _(i):
                attend_group(t * G_PER_CHUNK + i)

        @pl.when((t >= 1) & (t < N_CHUNKS + 1))
        def _():
            merge(0, t - 1)
            send(1, t - 1)

        @pl.when((t >= 2) & (t < N_CHUNKS + 2))
        def _():
            merge(1, t - 2)
            send(2, t - 2)

        @pl.when(t >= 3)
        def _():
            @pl.when(t == 3)
            def _():
                for h in range(HEADS):
                    wo_copy(h).wait()
            merge(2, t - 3)
            project_out(t - 3)

        @pl.when(t < N_CHUNKS)
        def _():
            @pl.loop(G_PER_CHUNK // 2, G_PER_CHUNK)
            def _(i):
                attend_group(t * G_PER_CHUNK + i)
            send(0, t)

    @pl.loop(0, N_CHUNKS)
    def _(k):
        for stage in range(3):
            for copy in exchange(stage, k):
                copy.wait_send()


def attend(hidden, w_norm, cos_t, sin_t, cache_len, w_q, w_k, w_v, w_o, k_block, v_block):
    vmem = pl.BlockSpec(memory_space=pltpu.VMEM)
    hbm = pl.BlockSpec(memory_space=pl.ANY)
    return pl.pallas_call(
        attend_kernel,
        out_shape=(jax.ShapeDtypeStruct((ROWS // 8, D), F32), jax.ShapeDtypeStruct((ROWS, HEAD), F32), jax.ShapeDtypeStruct((ROWS, HEAD), F32)),
        in_specs=[vmem, vmem, vmem, vmem, pl.BlockSpec(memory_space=pltpu.SMEM)] + [hbm] * 6,
        out_specs=(vmem, vmem, vmem),
        scratch_shapes=[
            pltpu.VMEM((D, D), BF16), pltpu.VMEM((2, D, HEAD), BF16), pltpu.VMEM((ROWS, D), BF16),
            pltpu.VMEM((2, ROWS * HEADS, HEAD // 2), F32),
            pltpu.VMEM((RING, GROUP, SLOTS, HEAD), BF16), pltpu.VMEM((RING, GROUP, SLOTS, HEAD), BF16),
            pltpu.VMEM((ROWS * HEADS, HEAD), F32), pltpu.VMEM((3 * N_CHUNKS, 2, HEADS, CHUNK), F32),
            pltpu.VMEM((N_CHUNKS, CHUNK // 2 * HEADS, HEAD), F32),
            pltpu.VMEM((N_CHUNKS, CHUNK // 4 * HEADS, HEAD), F32),
            pltpu.VMEM((N_CHUNKS, EIGHTH * HEADS, HEAD), F32),
            pltpu.VMEM((N_CHUNKS, 2, HEADS, CHUNK), F32), pltpu.VMEM((N_CHUNKS, 2, HEADS, CHUNK), F32), pltpu.VMEM((N_CHUNKS, 2, HEADS, CHUNK), F32),
            pltpu.VMEM((2, EIGHTH * HEADS, HEAD // 2), F32),
            pltpu.SemaphoreType.DMA((HEADS,)), pltpu.SemaphoreType.DMA((2,)),
            pltpu.SemaphoreType.DMA((RING,)), pltpu.SemaphoreType.DMA((RING,)),
            pltpu.SemaphoreType.DMA((3, N_CHUNKS)), pltpu.SemaphoreType.DMA((3, N_CHUNKS)),
            pltpu.SemaphoreType.DMA((3, N_CHUNKS)), pltpu.SemaphoreType.DMA((3, N_CHUNKS)),
        ],
        compiler_params=pltpu.CompilerParams(collective_id=0, has_side_effects=True, vmem_limit_bytes=60 * 2 ** 20),
        cost_estimate=pl.CostEstimate(flops=20 * 10 ** 9, bytes_accessed=90 * 10 ** 6, transcendentals=0),
    )(hidden, w_norm, cos_t, sin_t, cache_len, w_q, w_k, w_v, w_o, k_block, v_block)


COPY_RING = 8


def cache_kernel(len_ref, knew_ref, vnew_ref, k_hbm, v_hbm, ko_hbm, vo_hbm, buf, in_sem, out_sem):
    base = lax.axis_index('sp') * SLOTS
    sub16 = lax.broadcasted_iota(jnp.int32, (16, HEAD), 0)

    def ins(g):
        slot, rows = g % COPY_RING, pl.ds(g * GROUP, GROUP)
        return [pltpu.make_async_copy(src.at[rows], buf.at[i, slot], in_sem.at[i, slot]) for i, src in enumerate((k_hbm, v_hbm))]

    def outs(g):
        slot, rows = g % COPY_RING, pl.ds(g * GROUP, GROUP)
        return [pltpu.make_async_copy(buf.at[i, slot], dst.at[rows], out_sem.at[i, slot]) for i, dst in enumerate((ko_hbm, vo_hbm))]

    ahead = COPY_RING // 2
    for g in range(ahead):
        for copy in ins(g):
            copy.start()

    @pl.loop(0, N_GROUPS)
    def _(g):
        @pl.when(g + ahead < N_GROUPS)
        def _():
            @pl.when(g + ahead >= COPY_RING)
            def _():
                for copy in outs(g + ahead - COPY_RING):
                    copy.wait()
            for copy in ins(g + ahead):
                copy.start()
        for copy in ins(g):
            copy.wait()
        slot = g % COPY_RING
        for j in range(GROUP):
            r = g * GROUP + j
            at = len_ref[r] - base
            tile = jnp.clip(at, 0, SLOTS - 1) // 16 * 16
            span = pl.ds(pl.multiple_of(tile, 16), 16)
            hit = sub16 == at - tile
            for i, new_ref in enumerate((knew_ref, vnew_ref)):
                new = jnp.broadcast_to(new_ref[pl.ds(r, 1), :], (16, HEAD))
                old = buf[i, slot, j, span, :].astype(F32)
                buf[i, slot, j, span, :] = jnp.where(hit, new, old).astype(BF16)
        for copy in outs(g):
            copy.start()

    @pl.loop(N_GROUPS - COPY_RING, N_GROUPS)
    def _(g):
        for copy in outs(g):
            copy.wait()


def update_caches(cache_len, k_new, v_new, k_block, v_block):
    vmem = pl.BlockSpec(memory_space=pltpu.VMEM)
    hbm = pl.BlockSpec(memory_space=pl.ANY)
    shape = jax.ShapeDtypeStruct(k_block.shape, k_block.dtype)
    return pl.pallas_call(
        cache_kernel,
        out_shape=(shape, shape),
        in_specs=[pl.BlockSpec(memory_space=pltpu.SMEM), vmem, vmem, hbm, hbm],
        out_specs=(hbm, hbm),
        scratch_shapes=[pltpu.VMEM((2, COPY_RING, GROUP, SLOTS, HEAD), BF16), pltpu.SemaphoreType.DMA((2, COPY_RING)), pltpu.SemaphoreType.DMA((2, COPY_RING))],
        compiler_params=pltpu.CompilerParams(vmem_limit_bytes=40 * 2 ** 20),
        cost_estimate=pl.CostEstimate(flops=20 * 10 ** 9, bytes_accessed=134 * 10 ** 6, transcendentals=0),
    )(cache_len, k_new, v_new, k_block, v_block)


PIECES = (0, 2, 4, 6, 1, 3, 5, 7)


def assemble_kernel(*refs):
    pieces, out_ref = refs[:8], refs[8]
    me = lax.axis_index('sp')
    core, x, y = me % 2, (me // 2) % 2, me // 4
    for piece, flip in zip(pieces, PIECES):
        c = core + (flip % 2) * (1 - 2 * core)
        px = x + (flip // 2 % 2) * (1 - 2 * x)
        py = y + (flip // 4) * (1 - 2 * y)
        e = eighth_of(py * 4 + px * 2 + c)
        out_ref[pl.ds(pl.multiple_of(e * EIGHTH, EIGHTH), EIGHTH), :] = piece[...].astype(BF16)


def assemble(pieces):
    return pl.pallas_call(
        assemble_kernel,
        grid=(N_CHUNKS,),
        out_shape=jax.ShapeDtypeStruct((ROWS, D), BF16),
        in_specs=[pl.BlockSpec((EIGHTH, D), lambda k: (k, 0))] * 8,
        out_specs=pl.BlockSpec((CHUNK, D), lambda k: (k, 0)),
        cost_estimate=pl.CostEstimate(flops=10 ** 9, bytes_accessed=6 * 2 ** 20, transcendentals=0),
    )(*pieces)


def local_step(hidden, w_norm, w_q, w_k, w_v, w_o, k_block, v_block, cache_len):
    inv_freq = ROPE_BASE ** (-jnp.arange(HEAD // 2, dtype=F32) * 2.0 / HEAD)
    angles = cache_len.astype(F32)[:, None] * inv_freq[None, :]
    own, k_new, v_new = attend(hidden, w_norm[None, :], jnp.cos(angles), jnp.sin(angles), cache_len, w_q, w_k, w_v, w_o, k_block, v_block)

    def flip(array, bits):
        return lax.ppermute(array, 'sp', [(i, i ^ bits) for i in range(8)])

    held = [own] + [flip(own, bits) for bits in (2, 4, 6)]
    new_k, new_v = update_caches(cache_len, k_new, v_new, k_block, v_block)
    other = [flip(piece, 1) for piece in held]
    return assemble(held + other), new_k, new_v


def solution(mesh):
    cache_spec = P('dp', 'sp', None)
    return jax.shard_map(local_step, mesh=mesh, in_specs=(P('dp', None), P(None), P(None, None), P(None, None), P(None, None), P(None, None), cache_spec, cache_spec, P('dp')), out_specs=(P('dp', None), cache_spec, cache_spec), check_vma=False)
```

```python
import functools
import jax
import jax.numpy as jnp
import numpy as np
from jax import lax
from jax.experimental import pallas as pl
from jax.experimental.pallas import tpu as pltpu
from jax.sharding import PartitionSpec as P

ROPE_BASE = 10000.0
EPSILON = 1e-6
F32 = jnp.float32
BF16 = jnp.bfloat16
LOWEST = -3.0e38
MESH_ID = pl.DeviceIdType.MESH

ROWS, D, HEADS, HEAD, SLOTS = 512, 2048, 8, 256, 128
CHUNK = 128
N_CHUNKS = ROWS // CHUNK
GROUP = 16
N_GROUPS = ROWS // GROUP
G_PER_CHUNK = CHUNK // GROUP
RING = 16
EIGHTH = CHUNK // 8
X_ROWS = 128


def place(me):
    core = me % 2
    x = (me // 2) % 2
    y = me // 4
    partner = me + 1 - 2 * core
    x_peer = me + 2 * (1 - 2 * x)
    y_peer = me + 4 * (1 - 2 * y)
    first_bit = x + core * (y - x)
    second_bit = y + core * (x - y)
    first_peer = x_peer + core * (y_peer - x_peer)
    second_peer = y_peer + core * (x_peer - y_peer)
    return core, first_bit, second_bit, partner, first_peer, second_peer


def eighth_of(me):
    core, first_bit, second_bit, _, _, _ = place(me)
    return core * 4 + first_bit * 2 + second_bit


def dot(a, b):
    return jnp.dot(a, b, preferred_element_type=F32)


def attend_kernel(len_ref, freq_ref, wn_ref, x_hbm, wq_hbm, wk_hbm, wv_hbm, wo_hbm, k_hbm, v_hbm,
                  out_ref, knew_ref, vnew_ref, k_buf, v_buf,
                  w_buf, wkv_buf, xn_buf, x_own, cos_ref, sin_ref, q_buf, stat_buf, d_recv, f_recv, s_recv,
                  d_stat, f_stat, s_stat, p_buf, x_sem, own_sem, w_sem, wkv_sem, k_sem, v_sem, send_sem, recv_sem, ssend_sem, srecv_sem):
    me = lax.axis_index('sp')
    core, first_bit, second_bit, partner, first_peer, second_peer = place(me)
    base = me * SLOTS

    def wq_copy(h):
        cols = pl.ds(pl.multiple_of(h * HEAD, HEAD), HEAD)
        return pltpu.make_async_copy(wq_hbm.at[:, cols], w_buf.at[:, cols], w_sem.at[h])

    def wo_copy(h):
        rows = pl.ds(pl.multiple_of(h * HEAD, HEAD), HEAD)
        return pltpu.make_async_copy(wo_hbm.at[rows, :], w_buf.at[rows, :], w_sem.at[h])

    def cache_copies(g):
        slot = g % RING
        rows = pl.ds(g * GROUP, GROUP)
        return (pltpu.make_async_copy(k_hbm.at[rows], k_buf.at[slot], k_sem.at[slot]),
                pltpu.make_async_copy(v_hbm.at[rows], v_buf.at[slot], v_sem.at[slot]))

    def x_copy(i):
        rows = pl.ds(i * X_ROWS, X_ROWS)
        return pltpu.make_async_copy(x_hbm.at[rows, :], xn_buf.at[rows, :], x_sem.at[i])

    def own_copy(k):
        rows = pl.ds(pl.multiple_of(k * CHUNK + eighth_of(me) * EIGHTH, EIGHTH), EIGHTH)
        return pltpu.make_async_copy(x_hbm.at[rows, :], x_own.at[k], own_sem.at[k])

    for i in range(ROWS // X_ROWS):
        x_copy(i).start()
    wk_copy = pltpu.make_async_copy(wk_hbm, wkv_buf.at[0], wkv_sem.at[0])
    wv_copy = pltpu.make_async_copy(wv_hbm, wkv_buf.at[1], wkv_sem.at[1])
    for h in range(2):
        wq_copy(h).start()
    wk_copy.start()
    wv_copy.start()
    for h in range(2, HEADS):
        wq_copy(h).start()
    for k in range(N_CHUNKS):
        own_copy(k).start()
    for g in range(RING):
        for copy in cache_copies(g):
            copy.start()

    barrier = pltpu.get_barrier_semaphore()
    for peer in (partner, first_peer, second_peer):
        pl.semaphore_signal(barrier, inc=1, device_id={'sp': peer}, device_id_type=MESH_ID)
    pl.semaphore_wait(barrier, 3)

    @pl.loop(0, ROWS // 16)
    def _(i):
        for j in range(16):
            r = i * 16 + j
            cos_ref[pl.ds(r, 1), :] = len_ref[r].astype(F32) * freq_ref[...]

    @pl.loop(0, ROWS // 64)
    def _(i):
        rows = pl.ds(pl.multiple_of(i * 64, 64), 64)
        angles = cos_ref[rows, :]
        cos_ref[rows, :] = jnp.cos(angles)
        sin_ref[rows, :] = jnp.sin(angles)

    gain = 1.0 + wn_ref[...].astype(F32).reshape(1, D)

    @pl.loop(0, ROWS // X_ROWS)
    def _(n):
        x_copy(n).wait()

        @pl.loop(0, X_ROWS // 16)
        def _(i):
            rows = pl.ds(pl.multiple_of(n * X_ROWS + i * 16, 16), 16)
            x = xn_buf[rows, :].astype(F32)
            inv = lax.rsqrt(jnp.mean(x * x, axis=-1, keepdims=True) + EPSILON)
            xn_buf[rows, :] = (x * inv * gain).astype(BF16)

    def rotate(u, rows):
        u = u.astype(BF16).astype(F32)
        c, s = cos_ref[rows, :], sin_ref[rows, :]
        lo, hi = u[:, :HEAD // 2], u[:, HEAD // 2:]
        return lo * c - hi * s, hi * c + lo * s

    half = HEAD // 2
    row_tiles = [pl.ds(t * 256, 256) for t in range(ROWS // 256)]

    @pl.loop(0, HEADS)
    def _(h):
        wq_copy(h).wait()
        cols = pl.ds(pl.multiple_of(h * HEAD, HEAD), HEAD)
        for t, rows in enumerate(row_tiles):
            lo, hi = rotate(dot(xn_buf[rows, :], w_buf[:, cols]), rows)
            dst = pl.ds(t * 256 * HEADS + h, 256, stride=HEADS)
            q_buf[0, dst, :] = lo * HEAD ** -0.5
            q_buf[1, dst, :] = hi * HEAD ** -0.5

    wk_copy.wait()
    for rows in row_tiles:
        lo, hi = rotate(dot(xn_buf[rows, :], wkv_buf[0]), rows)
        knew_ref[rows, :half] = lo.astype(BF16).astype(F32)
        knew_ref[rows, half:] = hi.astype(BF16).astype(F32)
    wv_copy.wait()
    for rows in row_tiles:
        vnew_ref[rows, :] = dot(xn_buf[rows, :], wkv_buf[1]).astype(BF16).astype(F32)

    for h in range(HEADS):
        wo_copy(h).start()

    lane = lax.broadcasted_iota(jnp.int32, (HEADS, SLOTS), 1)
    sub16 = lax.broadcasted_iota(jnp.int32, (16, HEAD), 0).astype(F32).astype(BF16)

    def patched(ref, slot, j, new_row, lim):
        new = jnp.broadcast_to(new_row, (16, HEAD)).astype(BF16)
        tiles = []
        for t in range(SLOTS // 16):
            at = jnp.full((16, HEAD), (lim - t * 16).astype(F32), F32).astype(BF16)
            tiles.append(jnp.where(sub16 == at, new, ref[slot, j, t * 16:(t + 1) * 16, :]))
        return jnp.concatenate(tiles, axis=0)

    def attend_group(g):
        slot = g % RING
        for copy in cache_copies(g):
            copy.wait()
        chunk = g // G_PER_CHUNK

        UN = 8
        @pl.loop(0, GROUP // 2 // UN)
        def _(u):
            m_tile = stat_buf[chunk, 0]
            d_tile = stat_buf[chunk, 1]
            for pp in range(UN):
                pair = u * UN + pp
                r0 = g * GROUP + 2 * pair
                lims = [len_ref[r0 + a] - base for a in range(2)]
                keys = jnp.concatenate([patched(k_buf, slot, 2 * pair + a, knew_ref[pl.ds(r0 + a, 1), :], lims[a]) for a in range(2)], axis=0)
                q_rows = pl.ds(pl.multiple_of(r0 * HEADS, 16), 16)
                q2 = jnp.concatenate([q_buf[0, q_rows, :], q_buf[1, q_rows, :]], axis=1).astype(BF16)
                s2 = lax.dot_general(q2, keys, (((1,), (1,)), ((), ())), preferred_element_type=F32)
                probs = []
                for a in range(2):
                    s = s2[a * HEADS:(a + 1) * HEADS, a * SLOTS:(a + 1) * SLOTS]
                    valid = lane <= lims[a]
                    m = jnp.max(jnp.where(valid, s, LOWEST), axis=-1, keepdims=True)
                    p = jnp.where(valid, jnp.exp(s - m), 0.0)
                    den = jnp.sum(p, axis=-1, keepdims=True)
                    here = lane == (g % G_PER_CHUNK) * GROUP + 2 * pair + a
                    m_tile = jnp.where(here, m, m_tile)
                    d_tile = jnp.where(here, den, d_tile)
                    probs.append(p)
                zero = jnp.zeros((HEADS, SLOTS), F32)
                p2 = jnp.concatenate([jnp.concatenate([probs[0], zero], axis=1), jnp.concatenate([zero, probs[1]], axis=1)], axis=0).astype(BF16)
                p_buf[pair] = p2
            stat_buf[chunk, 0] = m_tile
            stat_buf[chunk, 1] = d_tile

        @pl.loop(0, GROUP // 2 // UN)
        def _(u):
            for pp in range(UN):
                pair = u * UN + pp
                r0 = g * GROUP + 2 * pair
                lims = [len_ref[r0 + a] - base for a in range(2)]
                values = jnp.concatenate([patched(v_buf, slot, 2 * pair + a, vnew_ref[pl.ds(r0 + a, 1), :], lims[a]) for a in range(2)], axis=0)
                o2 = dot(p_buf[pair], values)
                q_rows = pl.ds(pl.multiple_of(r0 * HEADS, 16), 16)
                q_buf[0, q_rows, :] = o2[:, :half]
                q_buf[1, q_rows, :] = o2[:, half:]
        @pl.when(g + RING < N_GROUPS)
        def _():
            for copy in cache_copies(g + RING):
                copy.start()

    def num_rows(k, offset, count):
        return pl.ds(pl.multiple_of((k * CHUNK + offset) * HEADS, 128), count * HEADS)

    half_rows, quarter_rows = CHUNK // 2, CHUNK // 4
    my_half = core * half_rows
    my_quarter = my_half + first_bit * quarter_rows
    my_eighth = my_quarter + second_bit * EIGHTH

    def exchange(stage, k):
        recv, stat, peer, offset, count = (
            (d_recv, d_stat, partner, (1 - core) * half_rows, half_rows),
            (f_recv, f_stat, first_peer, my_half + (1 - first_bit) * quarter_rows, quarter_rows),
            (s_recv, s_stat, second_peer, my_quarter + (1 - second_bit) * EIGHTH, EIGHTH))[stage]
        return (pltpu.make_async_remote_copy(
                    src_ref=q_buf.at[:, num_rows(k, offset, count), :], dst_ref=recv.at[k],
                    send_sem=send_sem.at[stage, k], recv_sem=recv_sem.at[stage, k],
                    device_id={'sp': peer}, device_id_type=MESH_ID),
                pltpu.make_async_remote_copy(
                    src_ref=stat_buf.at[stage * N_CHUNKS + k], dst_ref=stat.at[k],
                    send_sem=ssend_sem.at[stage, k], recv_sem=srecv_sem.at[stage, k],
                    device_id={'sp': peer}, device_id_type=MESH_ID))

    def merge(stage, k):
        recv, stat, offset, count = (
            (d_recv, d_stat, my_half, half_rows),
            (f_recv, f_stat, my_quarter, quarter_rows),
            (s_recv, s_stat, my_eighth, EIGHTH))[stage]
        for copy in exchange(stage, k):
            copy.wait_recv()
        m_a, d_a = stat_buf[stage * N_CHUNKS + k, 0], stat_buf[stage * N_CHUNKS + k, 1]
        m_b, d_b = stat[k, 0], stat[k, 1]
        m = jnp.maximum(m_a, m_b)
        f_a, f_b = jnp.exp(m_a - m), jnp.exp(m_b - m)
        den = d_a * f_a + d_b * f_b
        last = stage == 2
        if last:
            f_a, f_b = f_a / den, f_b / den
        else:
            stat_buf[(stage + 1) * N_CHUNKS + k, 0] = m
            stat_buf[(stage + 1) * N_CHUNKS + k, 1] = den
        shift = (CHUNK - offset) % CHUNK
        f_a = pltpu.roll(f_a, shift, 1)
        f_b = pltpu.roll(f_b, shift, 1)
        start = (k * CHUNK + offset) * HEADS
        for r in range(count):
            dst = pl.ds(pl.multiple_of(start + r * HEADS, HEADS), HEADS)
            a, b = f_a[:, r:r + 1], f_b[:, r:r + 1]
            for i in range(2):
                q_buf[i, dst, :] = q_buf[i, dst, :] * a + recv[k, i, r * HEADS:(r + 1) * HEADS, :] * b

    def send(stage, k):
        for copy in exchange(stage, k):
            copy.start()

    def project_out(k):
        atts = []
        for h in range(HEADS):
            heads = pl.ds((k * CHUNK + my_eighth) * HEADS + h, EIGHTH, stride=HEADS)
            atts.append(jnp.concatenate([q_buf[0, heads, :], q_buf[1, heads, :]], axis=1).astype(BF16))
        own_copy(k).wait()
        o_rows = pl.ds(pl.multiple_of(k * EIGHTH, EIGHTH), EIGHTH)
        for n in range(D // 512):
            cols = slice(n * 512, (n + 1) * 512)
            acc = dot(atts[0], w_buf[0:HEAD, cols])
            for h in range(1, HEADS):
                acc += dot(atts[h], w_buf[h * HEAD:(h + 1) * HEAD, cols])
            out_ref[o_rows, cols] = (x_own[k, :, cols].astype(F32) + acc).astype(BF16).astype(F32)

    @pl.loop(0, N_CHUNKS + 3)
    def _(t):
        @pl.when(t < N_CHUNKS)
        def _():
            @pl.loop(0, G_PER_CHUNK // 2)
            def _(i):
                attend_group(t * G_PER_CHUNK + i)

        @pl.when((t >= 1) & (t < N_CHUNKS + 1))
        def _():
            merge(0, t - 1)
            send(1, t - 1)

        @pl.when((t >= 2) & (t < N_CHUNKS + 2))
        def _():
            merge(1, t - 2)
            send(2, t - 2)

        @pl.when(t >= 3)
        def _():
            @pl.when(t == 3)
            def _():
                for h in range(HEADS):
                    wo_copy(h).wait()
            merge(2, t - 3)
            project_out(t - 3)

        @pl.when(t < N_CHUNKS)
        def _():
            @pl.loop(G_PER_CHUNK // 2, G_PER_CHUNK)
            def _(i):
                attend_group(t * G_PER_CHUNK + i)
            send(0, t)

    @pl.loop(0, N_CHUNKS)
    def _(k):
        for stage in range(3):
            for copy in exchange(stage, k):
                copy.wait_send()


def attend(cache_len, inv_freq, w_norm, hidden, w_q, w_k, w_v, w_o, k_block, v_block):
    vmem = pl.BlockSpec(memory_space=pltpu.VMEM)
    hbm = pl.BlockSpec(memory_space=pl.ANY)
    return pl.pallas_call(
        attend_kernel,
        out_shape=(pltpu.VMEM((ROWS // 8, D), F32), pltpu.VMEM((ROWS, HEAD), F32), pltpu.VMEM((ROWS, HEAD), F32),
                   pltpu.VMEM((RING, GROUP, SLOTS, HEAD), BF16), pltpu.VMEM((RING, GROUP, SLOTS, HEAD), BF16)),
        in_specs=[pl.BlockSpec(memory_space=pltpu.SMEM), vmem, vmem] + [hbm] * 7,
        out_specs=(vmem,) * 5,
        scratch_shapes=[
            pltpu.VMEM((D, D), BF16), pltpu.VMEM((2, D, HEAD), BF16), pltpu.VMEM((ROWS, D), BF16),
            pltpu.VMEM((N_CHUNKS, EIGHTH, D), BF16),
            pltpu.VMEM((ROWS, HEAD // 2), F32), pltpu.VMEM((ROWS, HEAD // 2), F32),
            pltpu.VMEM((2, ROWS * HEADS, HEAD // 2), F32), pltpu.VMEM((3 * N_CHUNKS, 2, HEADS, CHUNK), F32),
            pltpu.VMEM((N_CHUNKS, 2, CHUNK // 2 * HEADS, HEAD // 2), F32),
            pltpu.VMEM((N_CHUNKS, 2, CHUNK // 4 * HEADS, HEAD // 2), F32),
            pltpu.VMEM((N_CHUNKS, 2, EIGHTH * HEADS, HEAD // 2), F32),
            pltpu.VMEM((N_CHUNKS, 2, HEADS, CHUNK), F32), pltpu.VMEM((N_CHUNKS, 2, HEADS, CHUNK), F32), pltpu.VMEM((N_CHUNKS, 2, HEADS, CHUNK), F32),
            pltpu.VMEM((GROUP // 2, 16, 2 * SLOTS), BF16),
            pltpu.SemaphoreType.DMA((ROWS // X_ROWS,)), pltpu.SemaphoreType.DMA((N_CHUNKS,)),
            pltpu.SemaphoreType.DMA((HEADS,)), pltpu.SemaphoreType.DMA((2,)),
            pltpu.SemaphoreType.DMA((RING,)), pltpu.SemaphoreType.DMA((RING,)),
            pltpu.SemaphoreType.DMA((3, N_CHUNKS)), pltpu.SemaphoreType.DMA((3, N_CHUNKS)),
            pltpu.SemaphoreType.DMA((3, N_CHUNKS)), pltpu.SemaphoreType.DMA((3, N_CHUNKS)),
        ],
        compiler_params=pltpu.CompilerParams(collective_id=0, has_side_effects=True, vmem_limit_bytes=24 * 2 ** 20),
        cost_estimate=pl.CostEstimate(flops=20 * 10 ** 9, bytes_accessed=90 * 10 ** 6, transcendentals=0),
    )(cache_len, inv_freq, w_norm, hidden, w_q, w_k, w_v, w_o, k_block, v_block)


COPY_RING = 8
N_STREAM = N_GROUPS - RING


def cache_kernel(len_ref, knew_ref, vnew_ref, k_held, v_held, k_hbm, v_hbm, ko_hbm, vo_hbm, buf, in_sem, out_sem, held_sem):
    base = lax.axis_index('sp') * SLOTS
    sub16 = lax.broadcasted_iota(jnp.int32, (16, HEAD), 0)
    held = (k_held, v_held)

    def ins(g):
        slot, rows = g % COPY_RING, pl.ds(g * GROUP, GROUP)
        return [pltpu.make_async_copy(src.at[rows], buf.at[i, slot], in_sem.at[i, slot]) for i, src in enumerate((k_hbm, v_hbm))]

    def outs(g):
        slot, rows = g % COPY_RING, pl.ds(g * GROUP, GROUP)
        return [pltpu.make_async_copy(buf.at[i, slot], dst.at[rows], out_sem.at[i, slot]) for i, dst in enumerate((ko_hbm, vo_hbm))]

    def held_outs(h):
        rows = pl.ds((N_STREAM + h) * GROUP, GROUP)
        return [pltpu.make_async_copy(held[i].at[(N_STREAM + h) % RING], dst.at[rows], held_sem.at[i, h]) for i, dst in enumerate((ko_hbm, vo_hbm))]

    def patch(g, i, ref, index):
        new_ref = (knew_ref, vnew_ref)[i]
        for j in range(GROUP):
            r = g * GROUP + j
            at = len_ref[r] - base
            tile = jnp.clip(at, 0, SLOTS - 1) // 16 * 16
            span = pl.ds(pl.multiple_of(tile, 16), 16)
            new = jnp.broadcast_to(new_ref[pl.ds(r, 1), :], (16, HEAD))
            where = (*index, j, span, slice(None))
            ref[where] = jnp.where(sub16 == at - tile, new, ref[where].astype(F32)).astype(BF16)

    ahead = COPY_RING // 2
    for g in range(ahead):
        for copy in ins(g):
            copy.start()

    @pl.loop(0, N_STREAM)
    def _(g):
        for i in range(2):
            patch(N_STREAM + g, i, held[i], ((N_STREAM + g) % RING,))
        for copy in held_outs(g):
            copy.start()

        @pl.when(g + ahead < N_STREAM)
        def _():
            @pl.when(g + ahead >= COPY_RING)
            def _():
                for copy in outs(g + ahead - COPY_RING):
                    copy.wait()
            for copy in ins(g + ahead):
                copy.start()
        for copy in ins(g):
            copy.wait()
        for i in range(2):
            patch(g, i, buf, (i, g % COPY_RING))
        for copy in outs(g):
            copy.start()

    @pl.loop(N_STREAM - COPY_RING, N_STREAM)
    def _(g):
        for copy in outs(g):
            copy.wait()

    @pl.loop(0, RING)
    def _(h):
        for copy in held_outs(h):
            copy.wait()


def update_caches(cache_len, k_new, v_new, k_held, v_held, k_block, v_block):
    vmem = pl.BlockSpec(memory_space=pltpu.VMEM)
    hbm = pl.BlockSpec(memory_space=pl.ANY)
    shape = jax.ShapeDtypeStruct(k_block.shape, k_block.dtype)
    k_new, v_new, k_held, v_held = [pltpu.with_memory_space_constraint(a, pltpu.VMEM) for a in (k_new, v_new, k_held, v_held)]
    return pl.pallas_call(
        cache_kernel,
        out_shape=(shape, shape),
        in_specs=[pl.BlockSpec(memory_space=pltpu.SMEM), vmem, vmem, vmem, vmem, hbm, hbm],
        out_specs=(hbm, hbm),
        scratch_shapes=[pltpu.VMEM((2, COPY_RING, GROUP, SLOTS, HEAD), BF16), pltpu.SemaphoreType.DMA((2, COPY_RING)), pltpu.SemaphoreType.DMA((2, COPY_RING)),
                        pltpu.SemaphoreType.DMA((2, RING))],
        compiler_params=pltpu.CompilerParams(vmem_limit_bytes=24 * 2 ** 20),
        cost_estimate=pl.CostEstimate(flops=20 * 10 ** 9, bytes_accessed=134 * 10 ** 6, transcendentals=0),
    )(cache_len, k_new, v_new, k_held, v_held, k_block, v_block)


PIECES = (0, 2, 4, 6, 1, 3, 5, 7)


def assemble_kernel(*refs):
    pieces, out_ref = refs[:8], refs[8]
    me = lax.axis_index('sp')
    core, x, y = me % 2, (me // 2) % 2, me // 4
    for piece, flip in zip(pieces, PIECES):
        c = core + (flip % 2) * (1 - 2 * core)
        px = x + (flip // 2 % 2) * (1 - 2 * x)
        py = y + (flip // 4) * (1 - 2 * y)
        e = eighth_of(py * 4 + px * 2 + c)
        out_ref[pl.ds(pl.multiple_of(e * EIGHTH, EIGHTH), EIGHTH), :] = piece[...].astype(BF16)


def assemble(pieces):
    return pl.pallas_call(
        assemble_kernel,
        grid=(N_CHUNKS,),
        out_shape=jax.ShapeDtypeStruct((ROWS, D), BF16),
        in_specs=[pl.BlockSpec((EIGHTH, D), lambda k: (k, 0))] * 8,
        out_specs=pl.BlockSpec((CHUNK, D), lambda k: (k, 0)),
        cost_estimate=pl.CostEstimate(flops=10 ** 9, bytes_accessed=6 * 2 ** 20, transcendentals=0),
    )(*pieces)


def local_step(hidden, w_norm, w_q, w_k, w_v, w_o, k_block, v_block, cache_len):
    inv_freq = np.float32(ROPE_BASE) ** (-np.arange(HEAD // 2, dtype=np.float32) * np.float32(2.0 / HEAD))
    own, k_new, v_new, k_held, v_held = attend(cache_len, inv_freq[None, :], w_norm, hidden, w_q, w_k, w_v, w_o, k_block, v_block)

    def flip(array, bits):
        return lax.ppermute(array, 'sp', [(i, i ^ bits) for i in range(8)])

    held = [own] + [flip(own, bits) for bits in (2, 4, 6)]
    new_k, new_v = update_caches(cache_len, k_new, v_new, k_held, v_held, k_block, v_block)
    *held, new_k = lax.optimization_barrier((*held, new_k))
    other = [flip(piece, 1) for piece in held]
    return assemble(held + other), new_k, new_v


def solution(mesh):
    cache_spec = P('dp', 'sp', None)
    return jax.shard_map(local_step, mesh=mesh, in_specs=(P('dp', None), P(None), P(None, None), P(None, None), P(None, None), P(None, None), cache_spec, cache_spec, P('dp')), out_specs=(P('dp', None), cache_spec, cache_spec), check_vma=False)
```
